256 devices in a mesh: mem: 8 (over x, core), gx: 4 (over z_hi), gy: 8 (over z_lo, y).
Axes of the slice: x: 4, y: 4, z: 8 (z_hi: 4, z_lo: 2; z = z_hi * 2 + z_lo), core: 2. Of those that a mesh axis runs over, the one named last changes fastest.
Arguments:
- prior_sample_set: float32 [256, 2, 256, 1024], P('mem', None, 'gx', 'gy'), may hold values from -6 to 6
- flow_speeds: float32 [2, 2, 256, 1024], P(None, None, 'gx', 'gy'), may hold values from -0.6 to 0.6
- observed_cells: int32 [4, 8, 8, 4, 128], P('gx', 'gy', 'mem'), may hold values from 0 to 511
- observed_values: float32 [4, 8, 8, 4, 128], P('gx', 'gy', 'mem'), may hold values from -6 to 6
- error_variance: float32 [4, 8, 8, 4, 128], P('gx', 'gy', 'mem'), may hold values from 0.5 to 4
Outputs:
- analysis: bfloat16 [256, 2, 256, 1024], P('mem', None, 'gx', 'gy')
The draws below stay inside these ranges and needn't reach their ends.
All inputs are finite; a program needn't handle non-finite values.
Results may differ from the reference program's by a relative error of at most 0.001.
The reference program's roundings to bfloat16 on the way count: a program that leaves them out, or rounds other values in their place, can miss the bound.
Values may be sent and summed in bfloat16 or wider, within the bound.
A program may use at most 64 MiB of HBM per device.

```python
import math
import jax
import jax.numpy as jnp
from jax import lax

MEMBERS = 256
LAYERS = 2
RK_STEPS = 1
ROOT_STEPS = 4
PATCH = 256
OBS_PATCH = 128
STRIP = 1
NX = 256
NY = 1024
PATCHES = 4
N_MEM = 8
N_GX = 4
N_GY = 8


def plant(drawn, own_key, least, largest):
    extent = drawn.shape
    place = [jax.random.randint(jax.random.fold_in(own_key, axis), (), 0, extent[axis]) for axis in range(len(extent))]
    drawn = drawn.at[tuple(place)].set(least)
    longest = extent.index(max(extent))
    place[longest] = (place[longest] + 1) % extent[longest]
    return drawn.at[tuple(place)].set(largest)


def shard_levels(key, dims, shards, low, high):
    level, own = 1.0, jax.random.fold_in(key, 6)
    for axis_at, parts in shards:
        draws = jnp.exp(jax.random.uniform(jax.random.fold_in(own, axis_at), (parts,), jnp.float32, low / len(shards), high / len(shards)))
        level = level * jnp.repeat(draws, dims[axis_at] // parts).reshape([-1 if axis == axis_at else 1 for axis in range(len(dims))])
    return level


def scatter_about(key, extent, scale, bound, pieces=(), kind=jnp.bfloat16):
    factor_of = shard_levels(key, extent, pieces, -0.22, 0.18) if pieces else 1.0
    drawn = jax.random.normal(key, extent, jnp.float32) * scale * factor_of
    return jnp.minimum(jnp.maximum(drawn, -bound), bound).astype(kind)


def setup_inputs(seed: int = 0) -> dict:
    keys = jax.random.split(jax.random.key(seed), 6)
    return {
        "prior_sample_set": scatter_about(keys[0], (MEMBERS, LAYERS, NX, NY), 1.0, 6.0, ((0, 8), (2, 4), (3, 8)), jnp.float32),
        "flow_speeds": jnp.clip(jax.random.uniform(keys[1], (2, LAYERS, NX, NY), jnp.float32, -0.6, 0.6) * shard_levels(keys[1], (2, LAYERS, NX, NY), ((2, 4), (3, 8)), -0.4, 0.0), -0.6, 0.6),
        "observed_cells": plant(jax.random.randint(keys[2], (N_GX, N_GY, N_MEM, PATCHES, OBS_PATCH), 0, LAYERS * STRIP * PATCH), jax.random.fold_in(keys[2], 1), 0, (LAYERS * STRIP * PATCH) - 1).astype(jnp.int32),
        "observed_values": scatter_about(keys[3], (N_GX, N_GY, N_MEM, PATCHES, OBS_PATCH), 1.0, 6.0, ((0, 4), (1, 8), (2, 8)), jnp.float32),
        "error_variance": jnp.clip(jnp.exp(math.log(4.0) - 2.0794415 * jax.random.uniform(keys[4], (N_GX, N_GY, N_MEM, PATCHES, OBS_PATCH), jnp.float32) ** shard_levels(keys[4], (N_GX, N_GY, N_MEM, PATCHES, OBS_PATCH), ((0, 4), (1, 8), (2, 8)), -0.2, 0.2)), 0.5, 4.0),
    }


diffusion = 0.1
coupling = 0.2

def tendency(model_mesh_field, wind_x, wind_y):
    centre = model_mesh_field[:, :, 1:-1, 1:-1]
    north = model_mesh_field[:, :, 2:, 1:-1]
    south = model_mesh_field[:, :, :-2, 1:-1]
    east = model_mesh_field[:, :, 1:-1, 2:]
    west = model_mesh_field[:, :, 1:-1, :-2]
    layer_mean = lax.optimization_barrier(jnp.mean(centre, axis=1, keepdims=True))
    return -0.5 * wind_x * (north - south) - 0.5 * wind_y * (east - west) + diffusion * (north + south + east + west - 4.0 * centre) + coupling * (layer_mean - centre)

def wrap_section(model_mesh_field, flow_speeds):
    padded = jnp.pad(model_mesh_field, ((0, 0), (0, 0), (1, 1), (1, 1)), mode='wrap')
    return tendency(padded, flow_speeds[0], flow_speeds[1])

def wrap_step(model_mesh_field, flow_speeds):
    section_one = wrap_section(model_mesh_field, flow_speeds)
    section_two = wrap_section(model_mesh_field + 0.5 * section_one, flow_speeds)
    section_three = wrap_section(model_mesh_field + 0.5 * section_two, flow_speeds)
    section_four = wrap_section(model_mesh_field + section_three, flow_speeds)
    return model_mesh_field + (section_one + 2.0 * section_two + 2.0 * section_three + section_four) / 6.0

def advance_one_realization(realization_vector, flow_speeds):
    model_mesh_field = realization_vector[None]
    for step in range(RK_STEPS):
        model_mesh_field = wrap_step(model_mesh_field, flow_speeds)
    return model_mesh_field[0].astype(jnp.bfloat16)

def transform_exact(weights, rolled):
    return jnp.einsum('qik,ilsqc->klsqc', weights.astype(jnp.float32), rolled.astype(jnp.float32), precision=lax.Precision.HIGHEST)

def analyze(strip_block, cells, values, errors, transform):
    realization_vectors, layer_stack, rows, width = strip_block.shape
    patches, count = cells.shape
    patch = width // patches
    highest = lax.Precision.HIGHEST
    mean_field = lax.optimization_barrier(jnp.mean(strip_block, axis=0, dtype=jnp.float32))
    layer_of = cells // (rows * patch)
    row_of = cells // patch % rows
    column = cells % patch
    starts = (jnp.arange(patches, dtype=jnp.int32) * patch)[:, None]
    flat_index = (layer_of * (rows * width) + row_of * width + starts + column).astype(jnp.int32)
    picked = jnp.take(strip_block.reshape(realization_vectors, layer_stack * rows * width), flat_index.reshape(-1), axis=1)
    base = jnp.take(mean_field.reshape(-1), flat_index.reshape(-1)).reshape(patches, count)
    spread = picked.astype(jnp.float32).reshape(realization_vectors, patches, count) - base[None]
    innovation = values - base
    offset = column.astype(jnp.float32) - 0.5 * (patch - 1)
    spread_parts = []
    innovation_parts = []
    for shift in (-1, 0, 1):
        distance = (shift * patch + jnp.roll(offset, -shift, axis=0)) / patch
        scale = jnp.sqrt(jnp.exp(-0.5 * distance * distance) / jnp.roll(errors, -shift, axis=0))
        spread_parts.append(jnp.roll(spread, -shift, axis=1) * scale[None])
        innovation_parts.append(jnp.roll(innovation, -shift, axis=0) * scale)
    scaled = jnp.concatenate(spread_parts, axis=2)
    scaled_innovation = jnp.concatenate(innovation_parts, axis=1)
    identity = jnp.eye(realization_vectors, dtype=jnp.float32)
    gram = jnp.einsum('kpj,ipj->pki', scaled, scaled, precision=highest) + (realization_vectors - 1.0) * identity
    frob = jnp.sqrt(lax.optimization_barrier(jnp.sum(gram * gram, axis=(1, 2))))
    current = gram / frob[:, None, None]
    root = jnp.broadcast_to(identity, gram.shape)
    for step in range(ROOT_STEPS):
        middle = 1.5 * identity - 0.5 * jnp.einsum('pab,pbc->pac', root, current, precision=highest)
        current = jnp.einsum('pab,pbc->pac', current, middle, precision=highest)
        root = jnp.einsum('pab,pbc->pac', middle, root, precision=highest)
    projected = jnp.einsum('kpj,pj->pk', scaled, scaled_innovation, precision=highest)
    once = jnp.einsum('pab,pb->pa', root, projected, precision=highest)
    twice = jnp.einsum('pab,pb->pa', root, once, precision=highest)
    mean_weights = twice / frob[:, None]
    weights = (jnp.sqrt(realization_vectors - 1.0) * root / jnp.sqrt(frob)[:, None, None] + mean_weights[:, :, None]).astype(jnp.bfloat16)
    perturbation = (strip_block - mean_field[None]).astype(jnp.bfloat16)
    rolled = jnp.roll(perturbation, -(patch // 2), axis=3).reshape(realization_vectors, layer_stack, rows, patches, patch)
    first = transform(weights, rolled)
    second = transform(jnp.roll(weights, -1, axis=0), rolled)
    position = (jnp.arange(patch, dtype=jnp.float32) + 0.5) / patch
    increment = ((1.0 - position) * first + position * second).reshape(realization_vectors, layer_stack, rows, width)
    return (jnp.roll(increment, patch // 2, axis=3) + mean_field[None]).astype(jnp.bfloat16)

def reference(prior_sample_set, flow_speeds, observed_cells, observed_values, error_variance):
    realization_vectors = lax.map(lambda lone_element: advance_one_realization(lone_element, flow_speeds), prior_sample_set)
    strips = realization_vectors.reshape(MEMBERS, LAYERS, NX // STRIP, STRIP, NY).transpose(2, 0, 1, 3, 4)
    cells = observed_cells.reshape(NX // STRIP, PATCHES, OBS_PATCH)
    values = observed_values.reshape(NX // STRIP, PATCHES, OBS_PATCH)
    errors = error_variance.reshape(NX // STRIP, PATCHES, OBS_PATCH)

    def one_strip(items):
        return analyze(items[0], items[1], items[2], items[3], transform_exact)
    result = lax.map(one_strip, (strips, cells, values, errors))
    return result.transpose(1, 2, 0, 3, 4).reshape(MEMBERS, LAYERS, NX, NY)
```

```python
import functools

import jax
import jax.numpy as jnp
from jax import lax
from jax.experimental import pallas as pl
from jax.experimental.pallas import tpu as pltpu
from jax.sharding import PartitionSpec as P

MESH = pl.DeviceIdType.MESH
F32 = jnp.float32
BF16 = jnp.bfloat16

ROWS = 64
COLS = 128
LOCAL = 32
MEMS = 256
PEERS = 64
TOP = 8


def lanes_of(shape):
    return lax.broadcasted_iota(jnp.int32, shape, len(shape) - 1)


def roll(x, shift):
    shift = shift % COLS
    return x if shift == 0 else pltpu.roll(x, shift, x.ndim - 1)


def for_each_peer(mem, gy, body):
    def step(k, carry):
        other_mem, other_gy = lax.rem(k, 8), lax.div(k, 8)

        @pl.when(jnp.logical_or(other_mem != mem, other_gy != gy))
        def _():
            body(k, other_mem, other_gy)

        return carry

    lax.fori_loop(0, PEERS, step, 0)


def forecast_kernel(
    x_ref, w_ref, r_ref,
    u, v1, v2, v3, tu, t1, t2, t3,
    sends, dense, dense_in, corner_in,
    wide, packed, folded, folded_in, wind_corner_in, tw,
    coef, tcoef, out,
    h_send, h_recv, a_send, a_recv,
):
    mem, gx, gy = lax.axis_index("mem"), lax.axis_index("gx"), lax.axis_index("gy")
    up, down = lax.rem(gx + 1, 4), lax.rem(gx + 3, 4)
    east, west = lax.rem(gy + 1, 8), lax.rem(gy + 7, 8)
    me = gy * 8 + mem

    barrier = pltpu.get_barrier_semaphore()
    for other_gx in (up, down):
        for other_gy in (gy, east, west):
            pl.semaphore_signal(
                barrier, inc=1, device_id={"gx": other_gx, "gy": other_gy}, device_id_type=MESH
            )
    for_each_peer(
        mem, gy,
        lambda k, om, og: pl.semaphore_signal(
            barrier, inc=1, device_id={"mem": om, "gy": og}, device_id_type=MESH
        ),
    )

    lane = lanes_of((8, COLS))
    lane3 = lanes_of((8, 8, COLS))
    lane16 = lanes_of((16, 8, COLS))
    laneb = lanes_of((ROWS, COLS))
    lanec = lanes_of((16, COLS))

    edge = jnp.zeros((ROWS, COLS), F32)
    for q in range(4):
        wind = w_ref[q]
        wide[q, pl.ds(TOP, ROWS), :] = wind
        edge = jnp.where(laneb // 8 == q, roll(wind, 8 * q + 4), edge)
    packed[...] = edge
    fold = edge[0:16]
    for a in range(1, 4):
        fold = jnp.where(lanec // 32 == a, roll(edge[16 * a : 16 * a + 16], 32 * a), fold)
    folded[...] = fold

    def turn(rb, carry):
        edge = jnp.zeros((8, 8, COLS), F32)
        for l in range(2):
            for g in range(4):
                j = 4 * l + g
                block = x_ref[g * 8 : g * 8 + 8, l, pl.ds(rb * 8, 8), :]
                block = jnp.swapaxes(block, 0, 1)
                u[pl.ds(TOP + rb * 8, 8), l, g * 8 : g * 8 + 8, :] = block
                edge = jnp.where(lane3 // 8 == j, roll(block, 8 * j + 4), edge)
        sends[pl.ds(rb * 8, 8)] = edge
        return carry

    lax.fori_loop(0, 8, turn, 0)

    d0 = jnp.where(lane16 < 64, sends[0:16], roll(sends[32:48], 64))
    d1 = jnp.where(lane16 < 64, sends[16:32], roll(sends[48:64], 64))
    low16 = lax.rem(lane16, 8) < 4
    dense[0] = jnp.where(low16, d0, roll(d1, 4))
    dense[1] = jnp.where(low16, roll(d1, -4), d0)

    pl.semaphore_wait(barrier, PEERS - 1 + 6)

    plan = []

    def add(src, dst, device):
        i = len(plan)
        plan.append(
            pltpu.make_async_remote_copy(
                src_ref=src, dst_ref=dst, send_sem=h_send.at[i], recv_sem=h_recv.at[i],
                device_id=device, device_id_type=MESH,
            )
        )

    add(u.at[pl.ds(TOP + ROWS - 4, 4)], u.at[pl.ds(TOP - 4, 4)], {"gx": up})
    add(u.at[pl.ds(TOP, 4)], u.at[pl.ds(TOP + ROWS, 4)], {"gx": down})
    add(dense.at[0], dense_in.at[0], {"gy": east})
    add(dense.at[1], dense_in.at[1], {"gy": west})
    add(w_ref.at[:, pl.ds(ROWS - 8, 8), :], wide.at[:, pl.ds(0, 8), :], {"gx": up})
    add(w_ref.at[:, pl.ds(0, 8), :], wide.at[:, pl.ds(TOP + ROWS, 8), :], {"gx": down})
    add(folded, folded_in.at[0], {"gy": east})
    add(folded, folded_in.at[1], {"gy": west})
    corners = ((up, east, ROWS - 4, ROWS - 8), (up, west, ROWS - 4, ROWS - 8), (down, east, 0, 0), (down, west, 0, 0))
    for i, (cx, cy, row, wrow) in enumerate(corners):
        add(sends.at[pl.ds(row, 4)], corner_in.at[i], {"gx": cx, "gy": cy})
        add(packed.at[pl.ds(wrow, 8)], wind_corner_in.at[i], {"gx": cx, "gy": cy})
    for copy in plan:
        copy.start()
    for copy in plan:
        copy.wait()

    east_in, west_in = dense_in[0], dense_in[1]
    for a in range(4):
        right = 64 * (a // 2)
        left_part = roll(east_in, right - 4 * (a % 2))
        right_part = roll(west_in, right + 4 * (a % 2))
        tu[pl.ds(TOP + 16 * a, 16)] = jnp.where(low16, left_part, right_part)
    low4 = low16[0:4]
    tu[pl.ds(TOP - 4, 4)] = jnp.where(low4, corner_in[0], corner_in[1])
    tu[pl.ds(TOP + ROWS, 4)] = jnp.where(low4, corner_in[2], corner_in[3])

    lowc = lax.rem(lanec, 8) < 4
    low8 = lax.rem(lane, 8) < 4
    for a in range(4):
        tw[pl.ds(TOP + 16 * a, 16), :] = jnp.where(
            lowc, roll(folded_in[0], -32 * a), roll(folded_in[1], -32 * a)
        )
    tw[0:8, :] = jnp.where(low8, wind_corner_in[0], wind_corner_in[1])
    tw[pl.ds(TOP + ROWS, 8), :] = jnp.where(low8, wind_corner_in[2], wind_corner_in[3])

    lanew = lanes_of((80, COLS))
    tw_all = tw[...]
    for d in range(2):
        spread = jnp.zeros((80, COLS), F32)
        for j in range(8):
            spread = jnp.where(lanew // 8 == j, roll(tw_all, 8 * (j - (2 * d + j // 4))), spread)
        tcoef[2 * d] = 0.1 - 0.5 * spread
        tcoef[2 * d + 1] = 0.1 + 0.5 * spread
        for l in range(2):
            wind = wide[2 * d + l]
            coef[4 * l + 2 * d] = 0.1 - 0.5 * wind
            coef[4 * l + 2 * d + 1] = 0.1 + 0.5 * wind

    def row_of(ref, q, r):
        return jnp.broadcast_to(ref[q, pl.ds(r, 1), :], (8, COLS))

    def slopes(src, tsrc, r, with_edge):
        tc = tsrc[r]
        to_west, to_east = tc, tc
        centre = [[src[r, l, g * 8 : g * 8 + 8, :] for g in range(4)] for l in range(2)]
        result = [[None] * 4, [None] * 4]
        for l in range(2):
            an, as_, ae, aw = (row_of(coef, 4 * l + i, r) for i in range(4))
            for g in range(4):
                j = 4 * l + g
                c = centre[l][g]
                outside = roll(tc, 124 - 8 * j)
                w = roll(jnp.where(lane == COLS - 1, outside, c), 1)
                e = roll(jnp.where(lane == 0, outside, c), -1)
                if with_edge:
                    inside = roll(c, 8 * j + 4)
                    to_west = jnp.where(lane == 8 * j + 3, inside, to_west)
                    to_east = jnp.where(lane == 8 * j + 4, inside, to_east)
                n = src[r + 1, l, g * 8 : g * 8 + 8, :]
                s = src[r - 1, l, g * 8 : g * 8 + 8, :]
                result[l][g] = (
                    (an * n + as_ * s) + (ae * e + aw * w) + (0.1 * centre[1 - l][g] - 0.5 * c)
                )
        if not with_edge:
            return centre, result, None, None
        an, as_, ae, aw = (row_of(tcoef, i, r) for i in range(4))
        other = jnp.where(lane < 32, roll(tc, -32), roll(tc, 32))
        edge = (
            (an * tsrc[r + 1] + as_ * tsrc[r - 1])
            + (ae * roll(to_east, -1) + aw * roll(to_west, 1))
            + (0.1 * other - 0.5 * tc)
        )
        return centre, result, tc, edge

    def stage(src, tsrc, dst, tdst, alpha):
        def block(b, carry):
            for i in range(8):
                r = TOP - 4 + b * 8 + i
                _, result, _, edge = slopes(src, tsrc, r, True)
                for l in range(2):
                    for g in range(4):
                        dst[r, l, g * 8 : g * 8 + 8, :] = (
                            u[r, l, g * 8 : g * 8 + 8, :] + alpha * result[l][g]
                        )
                tdst[r] = tu[r] + alpha * edge
            return carry

        lax.fori_loop(0, 9, block, 0)

    stage(u, tu, v1, t1, 0.5)
    stage(v1, t1, v2, t2, 0.5)
    stage(v2, t2, v3, t3, 1.0)

    def piece(row, other_mem, other_gy, index):
        return pltpu.make_async_remote_copy(
            src_ref=out.at[row],
            dst_ref=r_ref.at[gy, :, pl.ds(pl.multiple_of(mem * LOCAL, LOCAL), LOCAL), :],
            send_sem=a_send.at[row], recv_sem=a_recv.at[index],
            device_id={"mem": other_mem, "gy": other_gy}, device_id_type=MESH,
        )

    def send_block(b):
        for i in range(8):
            row = b * 8 + i

            @pl.when(row != me)
            def _():
                piece(row, i, b, me).start()

    def last(k, carry):
        b = lax.rem(gy + k, 8)

        @pl.when(k > 0)
        def _():
            send_block(lax.rem(gy + k + 7, 8))

        for i in range(8):
            r = TOP + b * 8 + i
            centre, result, _, _ = slopes(v3, t3, r, False)
            for l in range(2):
                parts = []
                for g in range(4):
                    at = (r, l, slice(g * 8, g * 8 + 8), slice(None))
                    total = (v1[at] + 2.0 * v2[at]) + (centre[l][g] - u[at])
                    parts.append(total * (1.0 / 3.0) + result[l][g] * (1.0 / 6.0))
                out[b * 8 + i, l] = jnp.concatenate(parts, axis=0).astype(BF16)
        return carry

    lax.fori_loop(0, 8, last, 0)
    r_ref[gy, :, pl.ds(pl.multiple_of(mem * LOCAL, LOCAL), LOCAL), :] = out[me]
    send_block(lax.rem(gy + 7, 8))

    for_each_peer(mem, gy, lambda k, om, og: piece(k, om, og, k).wait_recv())
    for_each_peer(mem, gy, lambda k, om, og: piece(k, om, og, k).wait_send())


def forecast(x, winds):
    vm = pltpu.VMEM
    big = vm((80, 2, LOCAL, COLS), F32)
    thin = vm((80, 8, COLS), F32)
    return pl.pallas_call(
        forecast_kernel,
        out_shape=jax.ShapeDtypeStruct((8, 2, MEMS, COLS), BF16),
        in_specs=[pl.BlockSpec(memory_space=pltpu.VMEM)] * 2,
        out_specs=pl.BlockSpec(memory_space=pltpu.VMEM),
        scratch_shapes=[
            big, big, big, big, thin, thin, thin, thin,
            vm((ROWS, 8, COLS), F32), vm((2, 16, 8, COLS), F32), vm((2, 16, 8, COLS), F32),
            vm((4, 4, 8, COLS), F32),
            vm((4, 80, COLS), F32), vm((ROWS, COLS), F32), vm((16, COLS), F32),
            vm((2, 16, COLS), F32), vm((4, 8, COLS), F32), vm((80, COLS), F32),
            vm((8, 80, COLS), F32), vm((4, 80, COLS), F32), vm((ROWS, 2, LOCAL, COLS), BF16),
            pltpu.SemaphoreType.DMA((16,)), pltpu.SemaphoreType.DMA((16,)),
            pltpu.SemaphoreType.DMA((PEERS,)), pltpu.SemaphoreType.DMA((PEERS,)),
        ],
        compiler_params=pltpu.CompilerParams(collective_id=0, has_side_effects=True),
        name="forecast",
    )(x, winds)


def split(x):
    high = x.astype(BF16)
    return high, (x - high.astype(F32)).astype(BF16)


def dot(a, b, dims=((1,), (0,))):
    return lax.dot_general(a, b, (dims, ((), ())), preferred_element_type=F32)


def analysis_kernel(
    r_ref, cell_ref, value_ref, error_ref, o_ref,
    pert, mean, spread, innovation, weights, out, send_sem, recv_sem,
):
    mem, gy = lax.axis_index("mem"), lax.axis_index("gy")
    me = gy * 8 + mem
    barrier = pltpu.get_barrier_semaphore()
    for_each_peer(
        mem, gy,
        lambda k, om, og: pl.semaphore_signal(
            barrier, inc=1, device_id={"mem": om, "gy": og}, device_id_type=MESH
        ),
    )

    def centre(t, carry):
        for l in range(2):
            x = r_ref[t, l].astype(F32)
            mu = jnp.sum(x, axis=0, keepdims=True) * (1.0 / MEMS)
            mean[t, l : l + 1, :] = mu
            pert[t, :, l * COLS : (l + 1) * COLS] = (x - mu).astype(BF16)
        return carry

    lax.fori_loop(0, 8, centre, 0)

    site = lax.broadcasted_iota(jnp.int32, (COLS, COLS), 0)

    def observe(p, carry):
        cell = cell_ref[p]
        picked = jnp.zeros((MEMS, COLS), F32)
        for h in range(2):
            for l in range(2):
                chosen = jnp.where(site + (l * 256 + h * 128) == cell, 1.0, 0.0).astype(BF16)
                picked = picked + dot(r_ref[2 * p + h, l], chosen)
        base = jnp.sum(picked, axis=0, keepdims=True) * (1.0 / MEMS)
        spread[p] = picked - base
        innovation[p] = value_ref[p] - base
        return carry

    lax.fori_loop(0, 4, observe, 0)

    row = lax.broadcasted_iota(jnp.int32, (MEMS, MEMS), 0)
    column = lax.broadcasted_iota(jnp.int32, (MEMS, MEMS), 1)

    def times(a, b):
        return (dot(a[0], b[0]) + dot(a[0], b[1])) + dot(a[1], b[0])

    def unit(value):
        return jnp.where(row == column, value, 0.0)

    def solve(p, carry):
        parts = []
        projected = jnp.zeros((MEMS, 1), F32)
        for q in (-1, 0, 1):
            other = lax.rem(p + q + 4, 4)
            offset = lax.rem(cell_ref[other], 256).astype(F32) - 127.5
            distance = (q * 256 + offset) * (1.0 / 256.0)
            scale = jnp.sqrt(jnp.exp(-0.5 * distance * distance) / error_ref[other])
            part = spread[other] * scale
            projected = projected + jnp.sum(
                part * (innovation[other] * scale), axis=1, keepdims=True
            )
            parts.append(part)
        high, low = split(jnp.concatenate(parts, axis=1))
        both = ((1,), (1,))
        gram = (dot(high, high, both) + dot(high, low, both)) + dot(low, high, both) + unit(255.0)
        square = jnp.sum(
            jnp.sum(gram * gram, axis=0, keepdims=True), axis=1, keepdims=True
        )
        frob = jnp.sqrt(square)
        y = gram / frob
        middle = unit(1.5) - 0.5 * y
        z = split(middle)
        y = split(times(split(y), z))
        for step in range(1, 4):
            m = split(unit(1.5) - 0.5 * times(z, y))
            if step < 3:
                y = split(times(y, m))
                z = split(times(m, z))
            else:
                root = times(m, z)
        once = jnp.sum(root * projected, axis=0, keepdims=True)
        twice = jnp.sum(root * once, axis=1, keepdims=True)
        shift = jnp.sum(unit(twice), axis=0, keepdims=True) / frob
        weights[p] = (root * (jnp.sqrt(jnp.full((1, 1), 255.0, F32)) / jnp.sqrt(frob)) + shift).astype(BF16)
        return carry

    lax.fori_loop(0, 4, solve, 0)

    pl.semaphore_wait(barrier, PEERS - 1)

    def piece(t, other_mem, index):
        return pltpu.make_async_remote_copy(
            src_ref=out.at[t, :, pl.ds(pl.multiple_of(other_mem * LOCAL, LOCAL), LOCAL), :],
            dst_ref=o_ref.at[me],
            send_sem=send_sem.at[t * 8 + other_mem], recv_sem=recv_sem.at[index],
            device_id={"mem": other_mem, "gy": t}, device_id_type=MESH,
        )

    def send_tile(t):
        for i in range(8):

            @pl.when(t * 8 + i != me)
            def _():
                piece(t, i, me).start()

    position = lanes_of((1, MEMS)) % COLS

    def update(k, carry):
        t = lax.rem(gy + k, 8)

        @pl.when(k > 0)
        def _():
            send_tile(lax.rem(gy + k + 7, 8))

        s = lax.rem(lax.div(t + 7, 2), 4)
        half = 1 - lax.rem(t, 2)
        share = ((position + 128 * half).astype(F32) + 0.5) * (1.0 / 256.0)
        first = dot(weights[s], pert[t])
        second = dot(weights[lax.rem(s + 1, 4)], pert[t])
        increment = (1.0 - share) * first + share * second
        for l in range(2):
            out[t, l] = (
                increment[:, l * COLS : (l + 1) * COLS] + mean[t, l : l + 1, :]
            ).astype(BF16)
        return carry

    lax.fori_loop(0, 8, update, 0)
    o_ref[me] = out[gy, :, pl.ds(pl.multiple_of(mem * LOCAL, LOCAL), LOCAL), :]
    send_tile(lax.rem(gy + 7, 8))
    for_each_peer(mem, gy, lambda k, om, og: piece(og, om, k).wait_recv())
    for_each_peer(mem, gy, lambda k, om, og: piece(og, om, k).wait_send())


def analysis(strip, cells, values, errors):
    vm = pltpu.VMEM
    return pl.pallas_call(
        analysis_kernel,
        out_shape=jax.ShapeDtypeStruct((ROWS, 2, LOCAL, COLS), BF16),
        in_specs=[pl.BlockSpec(memory_space=pltpu.VMEM)] * 4,
        out_specs=pl.BlockSpec(memory_space=pltpu.VMEM),
        scratch_shapes=[
            vm((8, MEMS, MEMS), BF16), vm((8, 8, COLS), F32), vm((4, MEMS, COLS), F32),
            vm((4, 1, COLS), F32), vm((4, MEMS, MEMS), BF16), vm((8, 2, MEMS, COLS), BF16),
            pltpu.SemaphoreType.DMA((PEERS,)), pltpu.SemaphoreType.DMA((PEERS,)),
        ],
        compiler_params=pltpu.CompilerParams(collective_id=1, has_side_effects=True),
        name="analysis",
    )(strip, cells, values, errors)


def on_device(prior_sample_set, flow_speeds, observed_cells, observed_values, error_variance):
    strip = forecast(prior_sample_set, flow_speeds.reshape(4, ROWS, COLS))
    shape = (4, 1, COLS)
    result = analysis(
        strip,
        observed_cells.reshape(shape),
        observed_values.reshape(shape),
        error_variance.reshape(shape),
    )
    return jnp.transpose(result, (2, 1, 0, 3))


def solution(mesh):
    in_specs = (
        P("mem", None, "gx", "gy"),
        P(None, None, "gx", "gy"),
        P("gx", "gy", "mem", None, None),
        P("gx", "gy", "mem", None, None),
        P("gx", "gy", "mem", None, None),
    )
    out_specs = P("mem", None, "gx", "gy")
    return jax.shard_map(
        on_device, mesh=mesh, in_specs=in_specs, out_specs=out_specs, check_vma=False
    )
```

```python
import functools

import jax
import jax.numpy as jnp
from jax import lax
from jax.experimental import pallas as pl
from jax.experimental.pallas import tpu as pltpu
from jax.sharding import PartitionSpec as P

MESH = pl.DeviceIdType.MESH
F32 = jnp.float32
BF16 = jnp.bfloat16

ROWS = 64
COLS = 128
LOCAL = 32
MEMS = 256
PEERS = 64
TOP = 8


def lanes_of(shape):
    return lax.broadcasted_iota(jnp.int32, shape, len(shape) - 1)


def roll(x, shift):
    shift = shift % COLS
    return x if shift == 0 else pltpu.roll(x, shift, x.ndim - 1)


def mirrored(low, low_shift, high, high_shift):
    k_of = lanes_of(low.shape) % 8
    result = None
    for k in range(8):
        source, shift = (high, high_shift) if k < 4 else (low, low_shift)
        moved = roll(source, shift + 2 * k - 7)
        result = moved if k == 0 else jnp.where(k_of == k, moved, result)
    return result


def for_each_peer(mem, gy, body):
    def step(k, carry):
        other_mem, other_gy = lax.rem(k, 8), lax.div(k, 8)

        @pl.when(jnp.logical_or(other_mem != mem, other_gy != gy))
        def _():
            body(k, other_mem, other_gy)

        return carry

    lax.fori_loop(0, PEERS, step, 0)


def forecast_kernel(
    x_ref, w_ref, r_ref,
    u, v1, v2, v3, tu, t1, t2, t3,
    sends, dense, dense_in, corner_in,
    wide, packed, folded, folded_in, wind_corner_in, tw,
    coef, tcoef, out,
    h_send, h_recv, a_send, a_recv,
):
    mem, gx, gy = lax.axis_index("mem"), lax.axis_index("gx"), lax.axis_index("gy")
    up, down = lax.rem(gx + 1, 4), lax.rem(gx + 3, 4)
    east, west = lax.rem(gy + 1, 8), lax.rem(gy + 7, 8)
    me = gy * 8 + mem

    barrier = pltpu.get_barrier_semaphore()
    for other_gx in (up, down):
        for other_gy in (gy, east, west):
            pl.semaphore_signal(
                barrier, inc=1, device_id={"gx": other_gx, "gy": other_gy}, device_id_type=MESH
            )
    for_each_peer(
        mem, gy,
        lambda k, om, og: pl.semaphore_signal(
            barrier, inc=1, device_id={"mem": om, "gy": og}, device_id_type=MESH
        ),
    )

    lane = lanes_of((8, COLS))
    lane3 = lanes_of((8, 8, COLS))
    lane16 = lanes_of((16, 8, COLS))
    laneb = lanes_of((ROWS, COLS))
    lanec = lanes_of((16, COLS))

    edge = jnp.zeros((ROWS, COLS), F32)
    for q in range(4):
        wind = w_ref[q]
        wide[q, pl.ds(TOP, ROWS), :] = wind
        edge = jnp.where(laneb // 8 == q, roll(wind, 8 * q + 4), edge)
    packed[...] = edge
    fold = edge[0:16]
    for a in range(1, 4):
        fold = jnp.where(lanec // 32 == a, roll(edge[16 * a : 16 * a + 16], 32 * a), fold)
    folded[...] = fold

    def turn(rb, carry):
        edge = jnp.zeros((8, 8, COLS), F32)
        for l in range(2):
            for g in range(4):
                j = 4 * l + g
                block = x_ref[g * 8 : g * 8 + 8, l, pl.ds(rb * 8, 8), :]
                block = jnp.swapaxes(block, 0, 1)
                u[pl.ds(TOP + rb * 8, 8), l, g * 8 : g * 8 + 8, :] = block
                edge = jnp.where(lane3 // 8 == j, roll(block, 8 * j + 4), edge)
        sends[pl.ds(rb * 8, 8)] = edge
        return carry

    lax.fori_loop(0, 8, turn, 0)

    d0 = jnp.where(lane16 < 64, sends[0:16], roll(sends[32:48], 64))
    d1 = jnp.where(lane16 < 64, sends[16:32], roll(sends[48:64], 64))
    low16 = lax.rem(lane16, 8) < 4
    dense[0] = jnp.where(low16, d0, roll(d1, 4))
    dense[1] = jnp.where(low16, roll(d1, -4), d0)

    pl.semaphore_wait(barrier, PEERS - 1 + 6)

    plan = []

    def add(src, dst, device):
        i = len(plan)
        plan.append(
            pltpu.make_async_remote_copy(
                src_ref=src, dst_ref=dst, send_sem=h_send.at[i], recv_sem=h_recv.at[i],
                device_id=device, device_id_type=MESH,
            )
        )

    add(u.at[pl.ds(TOP + ROWS - 4, 4)], u.at[pl.ds(TOP - 4, 4)], {"gx": up})
    add(u.at[pl.ds(TOP, 4)], u.at[pl.ds(TOP + ROWS, 4)], {"gx": down})
    add(dense.at[0], dense_in.at[0], {"gy": east})
    add(dense.at[1], dense_in.at[1], {"gy": west})
    add(w_ref.at[:, pl.ds(ROWS - 8, 8), :], wide.at[:, pl.ds(0, 8), :], {"gx": up})
    add(w_ref.at[:, pl.ds(0, 8), :], wide.at[:, pl.ds(TOP + ROWS, 8), :], {"gx": down})
    add(folded, folded_in.at[0], {"gy": east})
    add(folded, folded_in.at[1], {"gy": west})
    corners = ((up, east, ROWS - 4, ROWS - 8), (up, west, ROWS - 4, ROWS - 8), (down, east, 0, 0), (down, west, 0, 0))
    for i, (cx, cy, row, wrow) in enumerate(corners):
        add(sends.at[pl.ds(row, 4)], corner_in.at[i], {"gx": cx, "gy": cy})
        add(packed.at[pl.ds(wrow, 8)], wind_corner_in.at[i], {"gx": cx, "gy": cy})
    for copy in plan:
        copy.start()
    for copy in plan:
        copy.wait()

    for a in range(4):
        right = 64 * (a // 2)
        for i in range(16):
            tu[TOP + 16 * a + i] = mirrored(
                dense_in[0, i], right - 4 * (a % 2), dense_in[1, i], right + 4 * (a % 2)
            )
    for i in range(4):
        tu[TOP - 4 + i] = mirrored(corner_in[0, i], 0, corner_in[1, i], 0)
        tu[TOP + ROWS + i] = mirrored(corner_in[2, i], 0, corner_in[3, i], 0)
    for a in range(4):
        tw[pl.ds(TOP + 16 * a, 16), :] = mirrored(folded_in[0], -32 * a, folded_in[1], -32 * a)
    tw[0:8, :] = mirrored(wind_corner_in[0], 0, wind_corner_in[1], 0)
    tw[pl.ds(TOP + ROWS, 8), :] = mirrored(wind_corner_in[2], 0, wind_corner_in[3], 0)

    lanew = lanes_of((80, COLS))
    tw_all = tw[...]
    for d in range(2):
        spread = jnp.zeros((80, COLS), F32)
        for j in range(8):
            spread = jnp.where(lanew // 8 == j, roll(tw_all, 8 * (j - (2 * d + j // 4))), spread)
        tcoef[2 * d] = 0.1 - 0.5 * spread
        tcoef[2 * d + 1] = 0.1 + 0.5 * spread
        for l in range(2):
            wind = wide[2 * d + l]
            coef[4 * l + 2 * d] = 0.1 - 0.5 * wind
            coef[4 * l + 2 * d + 1] = 0.1 + 0.5 * wind

    def row_of(ref, q, r):
        return jnp.broadcast_to(ref[q, pl.ds(r, 1), :], (8, COLS))

    def slopes(src, tsrc, r, with_edge):
        tc = tsrc[r]
        if with_edge:
            to_west, to_east = roll(tc, -1), roll(tc, 1)
        centre = [[src[r, l, g * 8 : g * 8 + 8, :] for g in range(4)] for l in range(2)]
        result = [[None] * 4, [None] * 4]
        for l in range(2):
            an, as_, ae, aw = (row_of(coef, 4 * l + i, r) for i in range(4))
            for g in range(4):
                j = 4 * l + g
                c = centre[l][g]
                outside = roll(tc, -(8 * j + 4))
                w = jnp.where(lane == 0, outside, roll(c, 1))
                e = jnp.where(lane == COLS - 1, outside, roll(c, -1))
                if with_edge:
                    inside = roll(c, 8 * j + 4)
                    to_west = jnp.where(lane == 8 * j + 3, inside, to_west)
                    to_east = jnp.where(lane == 8 * j + 4, inside, to_east)
                n = src[r + 1, l, g * 8 : g * 8 + 8, :]
                s = src[r - 1, l, g * 8 : g * 8 + 8, :]
                result[l][g] = (
                    (an * n + as_ * s) + (ae * e + aw * w) + (0.1 * centre[1 - l][g] - 0.5 * c)
                )
        if not with_edge:
            return centre, result, None, None
        an, as_, ae, aw = (row_of(tcoef, i, r) for i in range(4))
        other = jnp.where(lane < 32, roll(tc, -32), roll(tc, 32))
        edge = (
            (an * tsrc[r + 1] + as_ * tsrc[r - 1])
            + (ae * to_east + aw * to_west)
            + (0.1 * other - 0.5 * tc)
        )
        return centre, result, tc, edge

    def stage(src, tsrc, dst, tdst, alpha):
        def block(b, carry):
            for i in range(8):
                r = TOP - 4 + b * 8 + i
                _, result, _, edge = slopes(src, tsrc, r, True)
                for l in range(2):
                    for g in range(4):
                        dst[r, l, g * 8 : g * 8 + 8, :] = (
                            u[r, l, g * 8 : g * 8 + 8, :] + alpha * result[l][g]
                        )
                tdst[r] = tu[r] + alpha * edge
            return carry

        lax.fori_loop(0, 9, block, 0)

    stage(u, tu, v1, t1, 0.5)
    stage(v1, t1, v2, t2, 0.5)
    stage(v2, t2, v3, t3, 1.0)

    def piece(row, other_mem, other_gy, index):
        return pltpu.make_async_remote_copy(
            src_ref=out.at[row],
            dst_ref=r_ref.at[gy, :, pl.ds(pl.multiple_of(mem * LOCAL, LOCAL), LOCAL), :],
            send_sem=a_send.at[row], recv_sem=a_recv.at[index],
            device_id={"mem": other_mem, "gy": other_gy}, device_id_type=MESH,
        )

    def send_block(b):
        for i in range(8):
            row = b * 8 + i

            @pl.when(row != me)
            def _():
                piece(row, i, b, me).start()

    def last(k, carry):
        b = lax.rem(gy + k, 8)

        @pl.when(k > 0)
        def _():
            send_block(lax.rem(gy + k + 7, 8))

        for i in range(8):
            r = TOP + b * 8 + i
            centre, result, _, _ = slopes(v3, t3, r, False)
            for l in range(2):
                parts = []
                for g in range(4):
                    at = (r, l, slice(g * 8, g * 8 + 8), slice(None))
                    total = (v1[at] + 2.0 * v2[at]) + (centre[l][g] - u[at])
                    parts.append(total * (1.0 / 3.0) + result[l][g] * (1.0 / 6.0))
                out[b * 8 + i, l] = jnp.concatenate(parts, axis=0).astype(BF16)
        return carry

    lax.fori_loop(0, 8, last, 0)
    r_ref[gy, :, pl.ds(pl.multiple_of(mem * LOCAL, LOCAL), LOCAL), :] = out[me]
    send_block(lax.rem(gy + 7, 8))

    for_each_peer(mem, gy, lambda k, om, og: piece(k, om, og, k).wait_recv())
    for_each_peer(mem, gy, lambda k, om, og: piece(k, om, og, k).wait_send())


def forecast(x, winds):
    vm = pltpu.VMEM
    big = vm((80, 2, LOCAL, COLS), F32)
    thin = vm((80, 8, COLS), F32)
    return pl.pallas_call(
        forecast_kernel,
        out_shape=jax.ShapeDtypeStruct((8, 2, MEMS, COLS), BF16),
        in_specs=[pl.BlockSpec(memory_space=pltpu.VMEM)] * 2,
        out_specs=pl.BlockSpec(memory_space=pltpu.VMEM),
        scratch_shapes=[
            big, big, big, big, thin, thin, thin, thin,
            vm((ROWS, 8, COLS), F32), vm((2, 16, 8, COLS), F32), vm((2, 16, 8, COLS), F32),
            vm((4, 4, 8, COLS), F32),
            vm((4, 80, COLS), F32), vm((ROWS, COLS), F32), vm((16, COLS), F32),
            vm((2, 16, COLS), F32), vm((4, 8, COLS), F32), vm((80, COLS), F32),
            vm((8, 80, COLS), F32), vm((4, 80, COLS), F32), vm((ROWS, 2, LOCAL, COLS), BF16),
            pltpu.SemaphoreType.DMA((16,)), pltpu.SemaphoreType.DMA((16,)),
            pltpu.SemaphoreType.DMA((PEERS,)), pltpu.SemaphoreType.DMA((PEERS,)),
        ],
        compiler_params=pltpu.CompilerParams(collective_id=0, has_side_effects=True),
        name="forecast",
    )(x, winds)


def split(x):
    high = x.astype(BF16)
    return high, (x - high.astype(F32)).astype(BF16)


def dot(a, b, dims=((1,), (0,))):
    return lax.dot_general(a, b, (dims, ((), ())), preferred_element_type=F32)


def analysis_kernel(
    r_ref, cell_ref, value_ref, error_ref, o_ref,
    pert, mean, spread, innovation, weights, out, send_sem, recv_sem,
):
    mem, gy = lax.axis_index("mem"), lax.axis_index("gy")
    me = gy * 8 + mem
    barrier = pltpu.get_barrier_semaphore()
    for_each_peer(
        mem, gy,
        lambda k, om, og: pl.semaphore_signal(
            barrier, inc=1, device_id={"mem": om, "gy": og}, device_id_type=MESH
        ),
    )

    def centre(t, carry):
        for l in range(2):
            x = r_ref[t, l].astype(F32)
            mu = jnp.sum(x, axis=0, keepdims=True) * (1.0 / MEMS)
            mean[t, l : l + 1, :] = mu
            pert[t, :, l * COLS : (l + 1) * COLS] = (x - mu).astype(BF16)
        return carry

    lax.fori_loop(0, 8, centre, 0)

    site = lax.broadcasted_iota(jnp.int32, (COLS, COLS), 0)

    def observe(p, carry):
        cell = cell_ref[p]
        picked = jnp.zeros((MEMS, COLS), F32)
        for h in range(2):
            for l in range(2):
                chosen = jnp.where(site + (l * 256 + h * 128) == cell, 1.0, 0.0).astype(BF16)
                picked = picked + dot(r_ref[2 * p + h, l], chosen)
        base = jnp.sum(picked, axis=0, keepdims=True) * (1.0 / MEMS)
        spread[p] = picked - base
        innovation[p] = value_ref[p] - base
        return carry

    lax.fori_loop(0, 4, observe, 0)

    row = lax.broadcasted_iota(jnp.int32, (MEMS, MEMS), 0)
    column = lax.broadcasted_iota(jnp.int32, (MEMS, MEMS), 1)

    def times(a, b):
        return (dot(a[0], b[0]) + dot(a[0], b[1])) + dot(a[1], b[0])

    def unit(value):
        return jnp.where(row == column, value, 0.0)

    def solve(p, carry):
        parts = []
        projected = jnp.zeros((MEMS, 1), F32)
        for q in (-1, 0, 1):
            other = lax.rem(p + q + 4, 4)
            offset = lax.rem(cell_ref[other], 256).astype(F32) - 127.5
            distance = (q * 256 + offset) * (1.0 / 256.0)
            scale = jnp.sqrt(jnp.exp(-0.5 * distance * distance) / error_ref[other])
            part = spread[other] * scale
            projected = projected + jnp.sum(
                part * (innovation[other] * scale), axis=1, keepdims=True
            )
            parts.append(part)
        high, low = split(jnp.concatenate(parts, axis=1))
        both = ((1,), (1,))
        gram = (dot(high, high, both) + dot(high, low, both)) + dot(low, high, both) + unit(255.0)
        square = jnp.sum(
            jnp.sum(gram * gram, axis=0, keepdims=True), axis=1, keepdims=True
        )
        frob = jnp.sqrt(square)
        y = gram / frob
        middle = unit(1.5) - 0.5 * y
        z = split(middle)
        y = split(times(split(y), z))
        for step in range(1, 4):
            m = split(unit(1.5) - 0.5 * times(z, y))
            if step < 3:
                y = split(times(y, m))
                z = split(times(m, z))
            else:
                root = times(m, z)
        once = jnp.sum(root * projected, axis=0, keepdims=True)
        twice = jnp.sum(root * once, axis=1, keepdims=True)
        shift = jnp.sum(unit(twice), axis=0, keepdims=True) / frob
        weights[p] = (root * (jnp.sqrt(jnp.full((1, 1), 255.0, F32)) / jnp.sqrt(frob)) + shift).astype(BF16)
        return carry

    lax.fori_loop(0, 4, solve, 0)

    pl.semaphore_wait(barrier, PEERS - 1)

    def piece(t, other_mem, index):
        return pltpu.make_async_remote_copy(
            src_ref=out.at[t, :, pl.ds(pl.multiple_of(other_mem * LOCAL, LOCAL), LOCAL), :],
            dst_ref=o_ref.at[me],
            send_sem=send_sem.at[t * 8 + other_mem], recv_sem=recv_sem.at[index],
            device_id={"mem": other_mem, "gy": t}, device_id_type=MESH,
        )

    def send_tile(t):
        for i in range(8):

            @pl.when(t * 8 + i != me)
            def _():
                piece(t, i, me).start()

    position = lanes_of((1, MEMS)) % COLS

    def update(k, carry):
        t = lax.rem(gy + k, 8)

        @pl.when(k > 0)
        def _():
            send_tile(lax.rem(gy + k + 7, 8))

        s = lax.rem(lax.div(t + 7, 2), 4)
        half = 1 - lax.rem(t, 2)
        share = ((position + 128 * half).astype(F32) + 0.5) * (1.0 / 256.0)
        first = dot(weights[s], pert[t])
        second = dot(weights[lax.rem(s + 1, 4)], pert[t])
        increment = (1.0 - share) * first + share * second
        for l in range(2):
            out[t, l] = (
                increment[:, l * COLS : (l + 1) * COLS] + mean[t, l : l + 1, :]
            ).astype(BF16)
        return carry

    lax.fori_loop(0, 8, update, 0)
    o_ref[me] = out[gy, :, pl.ds(pl.multiple_of(mem * LOCAL, LOCAL), LOCAL), :]
    send_tile(lax.rem(gy + 7, 8))
    for_each_peer(mem, gy, lambda k, om, og: piece(og, om, k).wait_recv())
    for_each_peer(mem, gy, lambda k, om, og: piece(og, om, k).wait_send())


def analysis(strip, cells, values, errors):
    vm = pltpu.VMEM
    return pl.pallas_call(
        analysis_kernel,
        out_shape=jax.ShapeDtypeStruct((ROWS, 2, LOCAL, COLS), BF16),
        in_specs=[pl.BlockSpec(memory_space=pltpu.VMEM)] * 4,
        out_specs=pl.BlockSpec(memory_space=pltpu.VMEM),
        scratch_shapes=[
            vm((8, MEMS, MEMS), BF16), vm((8, 8, COLS), F32), vm((4, MEMS, COLS), F32),
            vm((4, 1, COLS), F32), vm((4, MEMS, MEMS), BF16), vm((8, 2, MEMS, COLS), BF16),
            pltpu.SemaphoreType.DMA((PEERS,)), pltpu.SemaphoreType.DMA((PEERS,)),
        ],
        compiler_params=pltpu.CompilerParams(collective_id=1, has_side_effects=True),
        name="analysis",
    )(strip, cells, values, errors)


def on_device(prior_sample_set, flow_speeds, observed_cells, observed_values, error_variance):
    strip = forecast(prior_sample_set, flow_speeds.reshape(4, ROWS, COLS))
    shape = (4, 1, COLS)
    result = analysis(
        strip,
        observed_cells.reshape(shape),
        observed_values.reshape(shape),
        error_variance.reshape(shape),
    )
    return jnp.transpose(result, (2, 1, 0, 3))


def solution(mesh):
    in_specs = (
        P("mem", None, "gx", "gy"),
        P(None, None, "gx", "gy"),
        P("gx", "gy", "mem", None, None),
        P("gx", "gy", "mem", None, None),
        P("gx", "gy", "mem", None, None),
    )
    out_specs = P("mem", None, "gx", "gy")
    return jax.shard_map(
        on_device, mesh=mesh, in_specs=in_specs, out_specs=out_specs, check_vma=False
    )
```

```python
import functools

import jax
import jax.numpy as jnp
from jax import lax
from jax.experimental import pallas as pl
from jax.experimental.pallas import tpu as pltpu
from jax.sharding import PartitionSpec as P

MESH = pl.DeviceIdType.MESH
F32 = jnp.float32
BF16 = jnp.bfloat16

ROWS = 64
COLS = 128
LOCAL = 32
MEMS = 256
PEERS = 64
TOP = 8


def lanes_of(shape):
    return lax.broadcasted_iota(jnp.int32, shape, len(shape) - 1)


def roll(x, shift):
    shift = shift % COLS
    return x if shift == 0 else pltpu.roll(x, shift, x.ndim - 1)


def mirrored(low, low_shift, high, high_shift):
    k_of = lanes_of(low.shape) % 8
    result = None
    for k in range(8):
        source, shift = (high, high_shift) if k < 4 else (low, low_shift)
        moved = roll(source, shift + 2 * k - 7)
        result = moved if k == 0 else jnp.where(k_of == k, moved, result)
    return result


def for_each_peer(mem, gy, body):
    def step(k, carry):
        other_mem, other_gy = lax.rem(k, 8), lax.div(k, 8)

        @pl.when(jnp.logical_or(other_mem != mem, other_gy != gy))
        def _():
            body(k, other_mem, other_gy)

        return carry

    lax.fori_loop(0, PEERS, step, 0)


def settle(pad):
    def step(i, carry):
        pad[...] = pad[...] * 0.5
        return carry

    lax.fori_loop(0, 40, step, 0)


def forecast_kernel(
    x_ref, w_ref, r_ref,
    u, v1, v2, v3, tu, t1, t2, t3,
    sends, dense, dense_in, corner_in,
    wide, packed, folded, folded_in, wind_corner_in, tw,
    coef, tcoef, out, pad,
    h_send, h_recv, a_send, a_recv,
):
    mem, gx, gy = lax.axis_index("mem"), lax.axis_index("gx"), lax.axis_index("gy")
    up, down = lax.rem(gx + 1, 4), lax.rem(gx + 3, 4)
    east, west = lax.rem(gy + 1, 8), lax.rem(gy + 7, 8)
    me = gy * 8 + mem

    barrier = pltpu.get_barrier_semaphore()
    for other_gx in (up, down):
        for other_gy in (gy, east, west):
            pl.semaphore_signal(
                barrier, inc=1, device_id={"gx": other_gx, "gy": other_gy}, device_id_type=MESH
            )
    for_each_peer(
        mem, gy,
        lambda k, om, og: pl.semaphore_signal(
            barrier, inc=1, device_id={"mem": om, "gy": og}, device_id_type=MESH
        ),
    )

    lane = lanes_of((8, COLS))
    lane3 = lanes_of((8, 8, COLS))
    lane16 = lanes_of((16, 8, COLS))
    laneb = lanes_of((ROWS, COLS))
    lanec = lanes_of((16, COLS))

    edge = jnp.zeros((ROWS, COLS), F32)
    for q in range(4):
        wind = w_ref[q]
        wide[q, pl.ds(TOP, ROWS), :] = wind
        edge = jnp.where(laneb // 8 == q, roll(wind, 8 * q + 4), edge)
    packed[...] = edge
    fold = edge[0:16]
    for a in range(1, 4):
        fold = jnp.where(lanec // 32 == a, roll(edge[16 * a : 16 * a + 16], 32 * a), fold)
    folded[...] = fold

    def turn(rb, carry):
        edge = jnp.zeros((8, 8, COLS), F32)
        for l in range(2):
            for g in range(4):
                j = 4 * l + g
                block = x_ref[g * 8 : g * 8 + 8, l, pl.ds(rb * 8, 8), :]
                block = jnp.swapaxes(block, 0, 1)
                u[pl.ds(TOP + rb * 8, 8), l, g * 8 : g * 8 + 8, :] = block
                edge = jnp.where(lane3 // 8 == j, roll(block, 8 * j + 4), edge)
        sends[pl.ds(rb * 8, 8)] = edge
        return carry

    lax.fori_loop(0, 8, turn, 0)

    d0 = jnp.where(lane16 < 64, sends[0:16], roll(sends[32:48], 64))
    d1 = jnp.where(lane16 < 64, sends[16:32], roll(sends[48:64], 64))
    low16 = lax.rem(lane16, 8) < 4
    dense[0] = jnp.where(low16, d0, roll(d1, 4))
    dense[1] = jnp.where(low16, roll(d1, -4), d0)

    settle(pad)
    pl.semaphore_wait(barrier, PEERS - 1 + 6)

    plan = []

    def add(src, dst, device):
        i = len(plan)
        plan.append(
            pltpu.make_async_remote_copy(
                src_ref=src, dst_ref=dst, send_sem=h_send.at[i], recv_sem=h_recv.at[i],
                device_id=device, device_id_type=MESH,
            )
        )

    add(u.at[pl.ds(TOP + ROWS - 4, 4)], u.at[pl.ds(TOP - 4, 4)], {"gx": up})
    add(u.at[pl.ds(TOP, 4)], u.at[pl.ds(TOP + ROWS, 4)], {"gx": down})
    add(dense.at[0], dense_in.at[0], {"gy": east})
    add(dense.at[1], dense_in.at[1], {"gy": west})
    add(w_ref.at[:, pl.ds(ROWS - 8, 8), :], wide.at[:, pl.ds(0, 8), :], {"gx": up})
    add(w_ref.at[:, pl.ds(0, 8), :], wide.at[:, pl.ds(TOP + ROWS, 8), :], {"gx": down})
    add(folded, folded_in.at[0], {"gy": east})
    add(folded, folded_in.at[1], {"gy": west})
    corners = ((up, east, ROWS - 4, ROWS - 8), (up, west, ROWS - 4, ROWS - 8), (down, east, 0, 0), (down, west, 0, 0))
    for i, (cx, cy, row, wrow) in enumerate(corners):
        add(sends.at[pl.ds(row, 4)], corner_in.at[i], {"gx": cx, "gy": cy})
        add(packed.at[pl.ds(wrow, 8)], wind_corner_in.at[i], {"gx": cx, "gy": cy})
    for copy in plan:
        copy.start()
    for copy in plan:
        copy.wait()

    for a in range(4):
        right = 64 * (a // 2)
        for i in range(16):
            tu[TOP + 16 * a + i] = mirrored(
                dense_in[0, i], right - 4 * (a % 2), dense_in[1, i], right + 4 * (a % 2)
            )
    for i in range(4):
        tu[TOP - 4 + i] = mirrored(corner_in[0, i], 0, corner_in[1, i], 0)
        tu[TOP + ROWS + i] = mirrored(corner_in[2, i], 0, corner_in[3, i], 0)
    for a in range(4):
        tw[pl.ds(TOP + 16 * a, 16), :] = mirrored(folded_in[0], -32 * a, folded_in[1], -32 * a)
    tw[0:8, :] = mirrored(wind_corner_in[0], 0, wind_corner_in[1], 0)
    tw[pl.ds(TOP + ROWS, 8), :] = mirrored(wind_corner_in[2], 0, wind_corner_in[3], 0)

    lanew = lanes_of((80, COLS))
    tw_all = tw[...]
    for d in range(2):
        spread = jnp.zeros((80, COLS), F32)
        for j in range(8):
            spread = jnp.where(lanew // 8 == j, roll(tw_all, 8 * (j - (2 * d + j // 4))), spread)
        tcoef[2 * d] = 0.1 - 0.5 * spread
        tcoef[2 * d + 1] = 0.1 + 0.5 * spread
        for l in range(2):
            wind = wide[2 * d + l]
            coef[4 * l + 2 * d] = 0.1 - 0.5 * wind
            coef[4 * l + 2 * d + 1] = 0.1 + 0.5 * wind

    def row_of(ref, q, r):
        return jnp.broadcast_to(ref[q, pl.ds(r, 1), :], (8, COLS))

    def slopes(src, tsrc, r, with_edge):
        tc = tsrc[r]
        if with_edge:
            to_west, to_east = roll(tc, -1), roll(tc, 1)
        centre = [[src[r, l, g * 8 : g * 8 + 8, :] for g in range(4)] for l in range(2)]
        result = [[None] * 4, [None] * 4]
        for l in range(2):
            an, as_, ae, aw = (row_of(coef, 4 * l + i, r) for i in range(4))
            for g in range(4):
                j = 4 * l + g
                c = centre[l][g]
                outside = roll(tc, -(8 * j + 4))
                w = jnp.where(lane == 0, outside, roll(c, 1))
                e = jnp.where(lane == COLS - 1, outside, roll(c, -1))
                if with_edge:
                    inside = roll(c, 8 * j + 4)
                    to_west = jnp.where(lane == 8 * j + 3, inside, to_west)
                    to_east = jnp.where(lane == 8 * j + 4, inside, to_east)
                n = src[r + 1, l, g * 8 : g * 8 + 8, :]
                s = src[r - 1, l, g * 8 : g * 8 + 8, :]
                result[l][g] = (
                    (an * n + as_ * s) + (ae * e + aw * w) + (0.1 * centre[1 - l][g] - 0.5 * c)
                )
        if not with_edge:
            return centre, result, None, None
        an, as_, ae, aw = (row_of(tcoef, i, r) for i in range(4))
        other = jnp.where(lane < 32, roll(tc, -32), roll(tc, 32))
        edge = (
            (an * tsrc[r + 1] + as_ * tsrc[r - 1])
            + (ae * to_east + aw * to_west)
            + (0.1 * other - 0.5 * tc)
        )
        return centre, result, tc, edge

    def stage(src, tsrc, dst, tdst, alpha):
        def block(b, carry):
            for i in range(8):
                r = TOP - 4 + b * 8 + i
                _, result, _, edge = slopes(src, tsrc, r, True)
                for l in range(2):
                    for g in range(4):
                        dst[r, l, g * 8 : g * 8 + 8, :] = (
                            u[r, l, g * 8 : g * 8 + 8, :] + alpha * result[l][g]
                        )
                tdst[r] = tu[r] + alpha * edge
            return carry

        lax.fori_loop(0, 9, block, 0)

    stage(u, tu, v1, t1, 0.5)
    stage(v1, t1, v2, t2, 0.5)
    stage(v2, t2, v3, t3, 1.0)

    def piece(row, other_mem, other_gy, index):
        return pltpu.make_async_remote_copy(
            src_ref=out.at[row],
            dst_ref=r_ref.at[gy, :, pl.ds(pl.multiple_of(mem * LOCAL, LOCAL), LOCAL), :],
            send_sem=a_send.at[row], recv_sem=a_recv.at[index],
            device_id={"mem": other_mem, "gy": other_gy}, device_id_type=MESH,
        )

    def send_block(b):
        for i in range(8):
            row = b * 8 + i

            @pl.when(row != me)
            def _():
                piece(row, i, b, me).start()

    def last(k, carry):
        b = lax.rem(gy + k, 8)

        @pl.when(k > 0)
        def _():
            settle(pad)
            send_block(lax.rem(gy + k + 7, 8))

        for i in range(8):
            r = TOP + b * 8 + i
            centre, result, _, _ = slopes(v3, t3, r, False)
            for l in range(2):
                parts = []
                for g in range(4):
                    at = (r, l, slice(g * 8, g * 8 + 8), slice(None))
                    total = (v1[at] + 2.0 * v2[at]) + (centre[l][g] - u[at])
                    parts.append(total * (1.0 / 3.0) + result[l][g] * (1.0 / 6.0))
                out[b * 8 + i, l] = jnp.concatenate(parts, axis=0).astype(BF16)
        return carry

    lax.fori_loop(0, 8, last, 0)
    r_ref[gy, :, pl.ds(pl.multiple_of(mem * LOCAL, LOCAL), LOCAL), :] = out[me]
    settle(pad)
    send_block(lax.rem(gy + 7, 8))

    for_each_peer(mem, gy, lambda k, om, og: piece(k, om, og, k).wait_recv())
    for_each_peer(mem, gy, lambda k, om, og: piece(k, om, og, k).wait_send())


def forecast(x, winds):
    vm = pltpu.VMEM
    big = vm((80, 2, LOCAL, COLS), F32)
    thin = vm((80, 8, COLS), F32)
    return pl.pallas_call(
        forecast_kernel,
        out_shape=jax.ShapeDtypeStruct((8, 2, MEMS, COLS), BF16),
        in_specs=[pl.BlockSpec(memory_space=pltpu.VMEM)] * 2,
        out_specs=pl.BlockSpec(memory_space=pltpu.VMEM),
        scratch_shapes=[
            big, big, big, big, thin, thin, thin, thin,
            vm((ROWS, 8, COLS), F32), vm((2, 16, 8, COLS), F32), vm((2, 16, 8, COLS), F32),
            vm((4, 4, 8, COLS), F32),
            vm((4, 80, COLS), F32), vm((ROWS, COLS), F32), vm((16, COLS), F32),
            vm((2, 16, COLS), F32), vm((4, 8, COLS), F32), vm((80, COLS), F32),
            vm((8, 80, COLS), F32), vm((4, 80, COLS), F32), vm((ROWS, 2, LOCAL, COLS), BF16), vm((8, COLS), F32),
            pltpu.SemaphoreType.DMA((16,)), pltpu.SemaphoreType.DMA((16,)),
            pltpu.SemaphoreType.DMA((PEERS,)), pltpu.SemaphoreType.DMA((PEERS,)),
        ],
        compiler_params=pltpu.CompilerParams(collective_id=0, has_side_effects=True),
        name="forecast",
    )(x, winds)


def split(x):
    high = x.astype(BF16)
    return high, (x - high.astype(F32)).astype(BF16)


def dot(a, b, dims=((1,), (0,))):
    return lax.dot_general(a, b, (dims, ((), ())), preferred_element_type=F32)


def analysis_kernel(
    r_ref, cell_ref, value_ref, error_ref, o_ref,
    pert, mean, spread, innovation, weights, out, pad, send_sem, recv_sem,
):
    mem, gy = lax.axis_index("mem"), lax.axis_index("gy")
    me = gy * 8 + mem
    barrier = pltpu.get_barrier_semaphore()
    for_each_peer(
        mem, gy,
        lambda k, om, og: pl.semaphore_signal(
            barrier, inc=1, device_id={"mem": om, "gy": og}, device_id_type=MESH
        ),
    )

    def centre(t, carry):
        for l in range(2):
            x = r_ref[t, l].astype(F32)
            mu = jnp.sum(x, axis=0, keepdims=True) * (1.0 / MEMS)
            mean[t, l : l + 1, :] = mu
            pert[t, :, l * COLS : (l + 1) * COLS] = (x - mu).astype(BF16)
        return carry

    lax.fori_loop(0, 8, centre, 0)

    site = lax.broadcasted_iota(jnp.int32, (COLS, COLS), 0)

    def observe(p, carry):
        cell = cell_ref[p]
        picked = jnp.zeros((MEMS, COLS), F32)
        for h in range(2):
            for l in range(2):
                chosen = jnp.where(site + (l * 256 + h * 128) == cell, 1.0, 0.0).astype(BF16)
                picked = picked + dot(r_ref[2 * p + h, l], chosen)
        base = jnp.sum(picked, axis=0, keepdims=True) * (1.0 / MEMS)
        spread[p] = picked - base
        innovation[p] = value_ref[p] - base
        return carry

    lax.fori_loop(0, 4, observe, 0)

    row = lax.broadcasted_iota(jnp.int32, (MEMS, MEMS), 0)
    column = lax.broadcasted_iota(jnp.int32, (MEMS, MEMS), 1)

    def times(a, b):
        return (dot(a[0], b[0]) + dot(a[0], b[1])) + dot(a[1], b[0])

    def unit(value):
        return jnp.where(row == column, value, 0.0)

    def solve(p):
        parts = []
        projected = jnp.zeros((MEMS, 1), F32)
        for q in (-1, 0, 1):
            other = lax.rem(p + q + 4, 4)
            offset = lax.rem(cell_ref[other], 256).astype(F32) - 127.5
            distance = (q * 256 + offset) * (1.0 / 256.0)
            scale = jnp.sqrt(jnp.exp(-0.5 * distance * distance) / error_ref[other])
            part = spread[other] * scale
            projected = projected + jnp.sum(
                part * (innovation[other] * scale), axis=1, keepdims=True
            )
            parts.append(part)
        high, low = split(jnp.concatenate(parts, axis=1))
        both = ((1,), (1,))
        gram = (dot(high, high, both) + dot(high, low, both)) + dot(low, high, both) + unit(255.0)
        square = jnp.sum(
            jnp.sum(gram * gram, axis=0, keepdims=True), axis=1, keepdims=True
        )
        frob = jnp.sqrt(square)
        y = gram / frob
        middle = unit(1.5) - 0.5 * y
        z = split(middle)
        y = split(times(split(y), z))
        for step in range(1, 4):
            m = split(unit(1.5) - 0.5 * times(z, y))
            if step < 3:
                y = split(times(y, m))
                z = split(times(m, z))
            else:
                root = times(m, z)
        once = jnp.sum(root * projected, axis=0, keepdims=True)
        twice = jnp.sum(root * once, axis=1, keepdims=True)
        shift = jnp.sum(unit(twice), axis=0, keepdims=True) / frob
        weights[p] = (root * (jnp.sqrt(jnp.full((1, 1), 255.0, F32)) / jnp.sqrt(frob)) + shift).astype(BF16)

    def piece(t, other_mem, index):
        return pltpu.make_async_remote_copy(
            src_ref=out.at[t, :, pl.ds(pl.multiple_of(other_mem * LOCAL, LOCAL), LOCAL), :],
            dst_ref=o_ref.at[me],
            send_sem=send_sem.at[t * 8 + other_mem], recv_sem=recv_sem.at[index],
            device_id={"mem": other_mem, "gy": t}, device_id_type=MESH,
        )

    def send_tile(t):
        for i in range(8):

            @pl.when(t * 8 + i != me)
            def _():
                piece(t, i, me).start()

    position = lanes_of((1, MEMS)) % COLS

    def update(s):
        tiles = []
        for h in range(2):
            half = lax.rem(gy + h, 2)
            t = lax.rem(2 * s + 1 + half, 8)
            share = ((position + 128 * half).astype(F32) + 0.5) * (1.0 / 256.0)
            first = dot(weights[s], pert[t])
            second = dot(weights[lax.rem(s + 1, 4)], pert[t])
            increment = (1.0 - share) * first + share * second
            for l in range(2):
                out[t, l] = (
                    increment[:, l * COLS : (l + 1) * COLS] + mean[t, l : l + 1, :]
                ).astype(BF16)
            tiles.append(t)
        settle(pad)
        for t in tiles:
            send_tile(t)

    def advance(k, carry):
        @pl.when(k < 4)
        def _():
            solve(lax.rem(lax.div(gy, 2) + k, 4))

        @pl.when(k == 0)
        def _():
            pl.semaphore_wait(barrier, PEERS - 1)

        @pl.when(k > 0)
        def _():
            update(lax.rem(lax.div(gy, 2) + k + 3, 4))

        return carry

    lax.fori_loop(0, 5, advance, 0)
    o_ref[me] = out[gy, :, pl.ds(pl.multiple_of(mem * LOCAL, LOCAL), LOCAL), :]
    for_each_peer(mem, gy, lambda k, om, og: piece(og, om, k).wait_recv())
    for_each_peer(mem, gy, lambda k, om, og: piece(og, om, k).wait_send())


def analysis(strip, cells, values, errors):
    vm = pltpu.VMEM
    return pl.pallas_call(
        analysis_kernel,
        out_shape=jax.ShapeDtypeStruct((ROWS, 2, LOCAL, COLS), BF16),
        in_specs=[pl.BlockSpec(memory_space=pltpu.VMEM)] * 4,
        out_specs=pl.BlockSpec(memory_space=pltpu.VMEM),
        scratch_shapes=[
            vm((8, MEMS, MEMS), BF16), vm((8, 8, COLS), F32), vm((4, MEMS, COLS), F32),
            vm((4, 1, COLS), F32), vm((4, MEMS, MEMS), BF16), vm((8, 2, MEMS, COLS), BF16), vm((8, COLS), F32),
            pltpu.SemaphoreType.DMA((PEERS,)), pltpu.SemaphoreType.DMA((PEERS,)),
        ],
        compiler_params=pltpu.CompilerParams(collective_id=1, has_side_effects=True),
        name="analysis",
    )(strip, cells, values, errors)


def on_device(prior_sample_set, flow_speeds, observed_cells, observed_values, error_variance):
    strip = forecast(prior_sample_set, flow_speeds.reshape(4, ROWS, COLS))
    shape = (4, 1, COLS)
    result = analysis(
        strip,
        observed_cells.reshape(shape),
        observed_values.reshape(shape),
        error_variance.reshape(shape),
    )
    return jnp.transpose(result, (2, 1, 0, 3))


def solution(mesh):
    in_specs = (
        P("mem", None, "gx", "gy"),
        P(None, None, "gx", "gy"),
        P("gx", "gy", "mem", None, None),
        P("gx", "gy", "mem", None, None),
        P("gx", "gy", "mem", None, None),
    )
    out_specs = P("mem", None, "gx", "gy")
    return jax.shard_map(
        on_device, mesh=mesh, in_specs=in_specs, out_specs=out_specs, check_vma=False
    )
```

```python
import functools

import jax
import jax.numpy as jnp
from jax import lax
from jax.experimental import pallas as pl
from jax.experimental.pallas import tpu as pltpu
from jax.sharding import PartitionSpec as P

MESH = pl.DeviceIdType.MESH
F32 = jnp.float32
BF16 = jnp.bfloat16

ROWS = 64
COLS = 128
LOCAL = 32
MEMS = 256
PEERS = 64
TOP = 8


def lanes_of(shape):
    return lax.broadcasted_iota(jnp.int32, shape, len(shape) - 1)


def roll(x, shift):
    shift = shift % COLS
    return x if shift == 0 else pltpu.roll(x, shift, x.ndim - 1)


def mirrored(low, low_shift, high, high_shift):
    k_of = lanes_of(low.shape) % 8
    result = None
    for k in range(8):
        source, shift = (high, high_shift) if k < 4 else (low, low_shift)
        moved = roll(source, shift + 2 * k - 7)
        result = moved if k == 0 else jnp.where(k_of == k, moved, result)
    return result


def for_each_peer(mem, gy, body):
    def step(k, carry):
        other_mem, other_gy = lax.rem(k, 8), lax.div(k, 8)

        @pl.when(jnp.logical_or(other_mem != mem, other_gy != gy))
        def _():
            body(k, other_mem, other_gy)

        return carry

    lax.fori_loop(0, PEERS, step, 0)


def settle(pad):
    def step(i, carry):
        pad[...] = pad[...] * 0.5
        return carry

    lax.fori_loop(0, 40, step, 0)


def forecast_kernel(
    x_ref, w_ref, r_ref,
    u, v1, v2, v3, tu, t1, t2, t3,
    sends, dense, dense_in, corner_in,
    wide, packed, folded, folded_in, wind_corner_in, tw,
    coef, tcoef, out, pad,
    h_send, h_recv, a_send, a_recv,
):
    mem, gx, gy = lax.axis_index("mem"), lax.axis_index("gx"), lax.axis_index("gy")
    up, down = lax.rem(gx + 1, 4), lax.rem(gx + 3, 4)
    east, west = lax.rem(gy + 1, 8), lax.rem(gy + 7, 8)
    me = gy * 8 + mem

    barrier = pltpu.get_barrier_semaphore()
    for other_gx in (up, down):
        for other_gy in (gy, east, west):
            pl.semaphore_signal(
                barrier, inc=1, device_id={"gx": other_gx, "gy": other_gy}, device_id_type=MESH
            )
    for_each_peer(
        mem, gy,
        lambda k, om, og: pl.semaphore_signal(
            barrier, inc=1, device_id={"mem": om, "gy": og}, device_id_type=MESH
        ),
    )

    lane = lanes_of((8, COLS))
    lane3 = lanes_of((8, 8, COLS))
    lane16 = lanes_of((16, 8, COLS))
    laneb = lanes_of((ROWS, COLS))
    lanec = lanes_of((16, COLS))

    edge = jnp.zeros((ROWS, COLS), F32)
    for q in range(4):
        wind = w_ref[q]
        wide[q, pl.ds(TOP, ROWS), :] = wind
        edge = jnp.where(laneb // 8 == q, roll(wind, 8 * q + 4), edge)
    packed[...] = edge
    fold = edge[0:16]
    for a in range(1, 4):
        fold = jnp.where(lanec // 32 == a, roll(edge[16 * a : 16 * a + 16], 32 * a), fold)
    folded[...] = fold

    def turn(rb, carry):
        edge = jnp.zeros((8, 8, COLS), F32)
        for l in range(2):
            for g in range(4):
                j = 4 * l + g
                block = x_ref[g * 8 : g * 8 + 8, l, pl.ds(rb * 8, 8), :]
                block = jnp.swapaxes(block, 0, 1)
                u[pl.ds(TOP + rb * 8, 8), l, g * 8 : g * 8 + 8, :] = block
                edge = jnp.where(lane3 // 8 == j, roll(block, 8 * j + 4), edge)
        sends[pl.ds(rb * 8, 8)] = edge
        return carry

    lax.fori_loop(0, 8, turn, 0)

    d0 = jnp.where(lane16 < 64, sends[0:16], roll(sends[32:48], 64))
    d1 = jnp.where(lane16 < 64, sends[16:32], roll(sends[48:64], 64))
    low16 = lax.rem(lane16, 8) < 4
    dense[0] = jnp.where(low16, d0, roll(d1, 4))
    dense[1] = jnp.where(low16, roll(d1, -4), d0)

    settle(pad)
    pl.semaphore_wait(barrier, PEERS - 1 + 6)

    plan = []

    def add(src, dst, device):
        i = len(plan)
        plan.append(
            pltpu.make_async_remote_copy(
                src_ref=src, dst_ref=dst, send_sem=h_send.at[i], recv_sem=h_recv.at[i],
                device_id=device, device_id_type=MESH,
            )
        )

    add(u.at[pl.ds(TOP + ROWS - 4, 4)], u.at[pl.ds(TOP - 4, 4)], {"gx": up})
    add(u.at[pl.ds(TOP, 4)], u.at[pl.ds(TOP + ROWS, 4)], {"gx": down})
    add(dense.at[0], dense_in.at[0], {"gy": east})
    add(dense.at[1], dense_in.at[1], {"gy": west})
    add(w_ref.at[:, pl.ds(ROWS - 8, 8), :], wide.at[:, pl.ds(0, 8), :], {"gx": up})
    add(w_ref.at[:, pl.ds(0, 8), :], wide.at[:, pl.ds(TOP + ROWS, 8), :], {"gx": down})
    add(folded, folded_in.at[0], {"gy": east})
    add(folded, folded_in.at[1], {"gy": west})
    corners = ((up, east, ROWS - 4, ROWS - 8), (up, west, ROWS - 4, ROWS - 8), (down, east, 0, 0), (down, west, 0, 0))
    for i, (cx, cy, row, wrow) in enumerate(corners):
        add(sends.at[pl.ds(row, 4)], corner_in.at[i], {"gx": cx, "gy": cy})
        add(packed.at[pl.ds(wrow, 8)], wind_corner_in.at[i], {"gx": cx, "gy": cy})
    for copy in plan:
        copy.start()
    for copy in plan:
        copy.wait()

    for a in range(4):
        right = 64 * (a // 2)
        for i in range(16):
            tu[TOP + 16 * a + i] = mirrored(
                dense_in[0, i], right - 4 * (a % 2), dense_in[1, i], right + 4 * (a % 2)
            )
    for i in range(4):
        tu[TOP - 4 + i] = mirrored(corner_in[0, i], 0, corner_in[1, i], 0)
        tu[TOP + ROWS + i] = mirrored(corner_in[2, i], 0, corner_in[3, i], 0)
    for a in range(4):
        tw[pl.ds(TOP + 16 * a, 16), :] = mirrored(folded_in[0], -32 * a, folded_in[1], -32 * a)
    tw[0:8, :] = mirrored(wind_corner_in[0], 0, wind_corner_in[1], 0)
    tw[pl.ds(TOP + ROWS, 8), :] = mirrored(wind_corner_in[2], 0, wind_corner_in[3], 0)

    lanew = lanes_of((80, COLS))
    tw_all = tw[...]
    for d in range(2):
        spread = jnp.zeros((80, COLS), F32)
        for j in range(8):
            spread = jnp.where(lanew // 8 == j, roll(tw_all, 8 * (j - (2 * d + j // 4))), spread)
        tcoef[2 * d] = 0.1 - 0.5 * spread
        tcoef[2 * d + 1] = 0.1 + 0.5 * spread
        for l in range(2):
            wind = wide[2 * d + l]
            coef[4 * l + 2 * d] = 0.1 - 0.5 * wind
            coef[4 * l + 2 * d + 1] = 0.1 + 0.5 * wind

    def row_of(ref, q, r):
        return jnp.broadcast_to(ref[q, pl.ds(r, 1), :], (8, COLS))

    def slopes(src, tsrc, r, with_edge):
        tc = tsrc[r]
        if with_edge:
            to_west, to_east = roll(tc, -1), roll(tc, 1)
        centre = [[src[r, l, g * 8 : g * 8 + 8, :] for g in range(4)] for l in range(2)]
        result = [[None] * 4, [None] * 4]
        for l in range(2):
            an, as_, ae, aw = (row_of(coef, 4 * l + i, r) for i in range(4))
            for g in range(4):
                j = 4 * l + g
                c = centre[l][g]
                outside = roll(tc, -(8 * j + 4))
                w = jnp.where(lane == 0, outside, roll(c, 1))
                e = jnp.where(lane == COLS - 1, outside, roll(c, -1))
                if with_edge:
                    inside = roll(c, 8 * j + 4)
                    to_west = jnp.where(lane == 8 * j + 3, inside, to_west)
                    to_east = jnp.where(lane == 8 * j + 4, inside, to_east)
                n = src[r + 1, l, g * 8 : g * 8 + 8, :]
                s = src[r - 1, l, g * 8 : g * 8 + 8, :]
                result[l][g] = (
                    (an * n + as_ * s) + (ae * e + aw * w) + (0.1 * centre[1 - l][g] - 0.5 * c)
                )
        if not with_edge:
            return centre, result, None, None
        an, as_, ae, aw = (row_of(tcoef, i, r) for i in range(4))
        other = jnp.where(lane < 32, roll(tc, -32), roll(tc, 32))
        edge = (
            (an * tsrc[r + 1] + as_ * tsrc[r - 1])
            + (ae * to_east + aw * to_west)
            + (0.1 * other - 0.5 * tc)
        )
        return centre, result, tc, edge

    def stage(first, src, tsrc, dst, tdst, alpha):
        for i in range(8):
            r = first + i
            _, result, _, edge = slopes(src, tsrc, r, True)
            for l in range(2):
                for g in range(4):
                    dst[r, l, g * 8 : g * 8 + 8, :] = (
                        u[r, l, g * 8 : g * 8 + 8, :] + alpha * result[l][g]
                    )
            tdst[r] = tu[r] + alpha * edge

    def piece(row, other_mem, other_gy, index):
        return pltpu.make_async_remote_copy(
            src_ref=out.at[row],
            dst_ref=r_ref.at[gy, :, pl.ds(pl.multiple_of(mem * LOCAL, LOCAL), LOCAL), :],
            send_sem=a_send.at[row], recv_sem=a_recv.at[index],
            device_id={"mem": other_mem, "gy": other_gy}, device_id_type=MESH,
        )

    def send_block(b):
        for i in range(8):
            row = b * 8 + i

            @pl.when(row != me)
            def _():
                piece(row, i, b, me).start()

    def finish(b):
        for i in range(8):
            r = TOP + b * 8 + i
            centre, result, _, _ = slopes(v3, t3, r, False)
            for l in range(2):
                parts = []
                for g in range(4):
                    at = (r, l, slice(g * 8, g * 8 + 8), slice(None))
                    total = (v1[at] + 2.0 * v2[at]) + (centre[l][g] - u[at])
                    parts.append(total * (1.0 / 3.0) + result[l][g] * (1.0 / 6.0))
                out[b * 8 + i, l] = jnp.concatenate(parts, axis=0).astype(BF16)

    ahead = 8 - gy

    def block_at(k):
        second = k > ahead
        block = jnp.where(second, k - ahead - 2, gy + k - 1)
        return block, jnp.logical_or(k == 0, k == ahead + 1)

    def advance(k, carry):
        b, filling = block_at(k)
        first = TOP + b * 8
        stage(first + 3, u, tu, v1, t1, 0.5)
        sent, no_send = block_at(k - 1)

        @pl.when(jnp.logical_and(k > 0, jnp.logical_not(no_send)))
        def _():
            send_block(sent)

        @pl.when(k + gy >= 0)
        def _():
            stage(first + 2, v1, t1, v2, t2, 0.5)

        @pl.when(k + mem >= 0)
        def _():
            stage(first + 1, v2, t2, v3, t3, 1.0)

        @pl.when(jnp.logical_not(filling))
        def _():
            finish(b)

        return carry

    steps = jnp.where(gy == 0, 9, 10)
    lax.fori_loop(0, steps, advance, 0)
    r_ref[gy, :, pl.ds(pl.multiple_of(mem * LOCAL, LOCAL), LOCAL), :] = out[me]
    settle(pad)
    send_block(lax.rem(gy + 7, 8))

    for_each_peer(mem, gy, lambda k, om, og: piece(k, om, og, k).wait_recv())
    for_each_peer(mem, gy, lambda k, om, og: piece(k, om, og, k).wait_send())


def forecast(x, winds):
    vm = pltpu.VMEM
    big = vm((80, 2, LOCAL, COLS), F32)
    thin = vm((80, 8, COLS), F32)
    return pl.pallas_call(
        forecast_kernel,
        out_shape=jax.ShapeDtypeStruct((8, 2, MEMS, COLS), BF16),
        in_specs=[pl.BlockSpec(memory_space=pltpu.VMEM)] * 2,
        out_specs=pl.BlockSpec(memory_space=pltpu.VMEM),
        scratch_shapes=[
            big, big, big, big, thin, thin, thin, thin,
            vm((ROWS, 8, COLS), F32), vm((2, 16, 8, COLS), F32), vm((2, 16, 8, COLS), F32),
            vm((4, 4, 8, COLS), F32),
            vm((4, 80, COLS), F32), vm((ROWS, COLS), F32), vm((16, COLS), F32),
            vm((2, 16, COLS), F32), vm((4, 8, COLS), F32), vm((80, COLS), F32),
            vm((8, 80, COLS), F32), vm((4, 80, COLS), F32), vm((ROWS, 2, LOCAL, COLS), BF16), vm((8, COLS), F32),
            pltpu.SemaphoreType.DMA((16,)), pltpu.SemaphoreType.DMA((16,)),
            pltpu.SemaphoreType.DMA((PEERS,)), pltpu.SemaphoreType.DMA((PEERS,)),
        ],
        compiler_params=pltpu.CompilerParams(collective_id=0, has_side_effects=True),
        name="forecast",
    )(x, winds)


def split(x):
    high = x.astype(BF16)
    return high, (x - high.astype(F32)).astype(BF16)


def dot(a, b, dims=((1,), (0,))):
    return lax.dot_general(a, b, (dims, ((), ())), preferred_element_type=F32)


def analysis_kernel(
    r_ref, cell_ref, value_ref, error_ref, o_ref,
    pert, mean, spread, innovation, weights, out, pad, send_sem, recv_sem,
):
    mem, gy = lax.axis_index("mem"), lax.axis_index("gy")
    me = gy * 8 + mem
    barrier = pltpu.get_barrier_semaphore()
    for_each_peer(
        mem, gy,
        lambda k, om, og: pl.semaphore_signal(
            barrier, inc=1, device_id={"mem": om, "gy": og}, device_id_type=MESH
        ),
    )

    def centre(t, carry):
        for l in range(2):
            x = r_ref[t, l].astype(F32)
            mu = jnp.sum(x, axis=0, keepdims=True) * (1.0 / MEMS)
            mean[t, l : l + 1, :] = mu
            pert[t, :, l * COLS : (l + 1) * COLS] = (x - mu).astype(BF16)
        return carry

    lax.fori_loop(0, 8, centre, 0)

    site = lax.broadcasted_iota(jnp.int32, (COLS, COLS), 0)

    def observe(p, carry):
        cell = cell_ref[p]
        picked = jnp.zeros((MEMS, COLS), F32)
        for h in range(2):
            for l in range(2):
                chosen = jnp.where(site + (l * 256 + h * 128) == cell, 1.0, 0.0).astype(BF16)
                picked = picked + dot(r_ref[2 * p + h, l], chosen)
        base = jnp.sum(picked, axis=0, keepdims=True) * (1.0 / MEMS)
        spread[p] = picked - base
        innovation[p] = value_ref[p] - base
        return carry

    lax.fori_loop(0, 4, observe, 0)

    row = lax.broadcasted_iota(jnp.int32, (MEMS, MEMS), 0)
    column = lax.broadcasted_iota(jnp.int32, (MEMS, MEMS), 1)

    def times(a, b):
        return (dot(a[0], b[0]) + dot(a[0], b[1])) + dot(a[1], b[0])

    def unit(value):
        return jnp.where(row == column, value, 0.0)

    def solve(p):
        parts = []
        projected = jnp.zeros((MEMS, 1), F32)
        for q in (-1, 0, 1):
            other = lax.rem(p + q + 4, 4)
            offset = lax.rem(cell_ref[other], 256).astype(F32) - 127.5
            distance = (q * 256 + offset) * (1.0 / 256.0)
            scale = jnp.sqrt(jnp.exp(-0.5 * distance * distance) / error_ref[other])
            part = spread[other] * scale
            projected = projected + jnp.sum(
                part * (innovation[other] * scale), axis=1, keepdims=True
            )
            parts.append(part)
        high, low = split(jnp.concatenate(parts, axis=1))
        both = ((1,), (1,))
        gram = (dot(high, high, both) + dot(high, low, both)) + dot(low, high, both) + unit(255.0)
        square = jnp.sum(
            jnp.sum(gram * gram, axis=0, keepdims=True), axis=1, keepdims=True
        )
        frob = jnp.sqrt(square)
        y = gram / frob
        middle = unit(1.5) - 0.5 * y
        z = split(middle)
        y = split(times(split(y), z))
        for step in range(1, 4):
            m = split(unit(1.5) - 0.5 * times(z, y))
            if step < 3:
                y = split(times(y, m))
                z = split(times(m, z))
            else:
                root = times(m, z)
        once = jnp.sum(root * projected, axis=0, keepdims=True)
        twice = jnp.sum(root * once, axis=1, keepdims=True)
        shift = jnp.sum(unit(twice), axis=0, keepdims=True) / frob
        weights[p] = (root * (jnp.sqrt(jnp.full((1, 1), 255.0, F32)) / jnp.sqrt(frob)) + shift).astype(BF16)

    def piece(t, other_mem, index):
        return pltpu.make_async_remote_copy(
            src_ref=out.at[t, :, pl.ds(pl.multiple_of(other_mem * LOCAL, LOCAL), LOCAL), :],
            dst_ref=o_ref.at[me],
            send_sem=send_sem.at[t * 8 + other_mem], recv_sem=recv_sem.at[index],
            device_id={"mem": other_mem, "gy": t}, device_id_type=MESH,
        )

    def send_tile(t):
        for i in range(8):

            @pl.when(t * 8 + i != me)
            def _():
                piece(t, i, me).start()

    position = lanes_of((1, MEMS)) % COLS

    def update(s):
        tiles = []
        for h in range(2):
            half = lax.rem(gy + h, 2)
            t = lax.rem(2 * s + 1 + half, 8)
            share = ((position + 128 * half).astype(F32) + 0.5) * (1.0 / 256.0)
            first = dot(weights[s], pert[t])
            second = dot(weights[lax.rem(s + 1, 4)], pert[t])
            increment = (1.0 - share) * first + share * second
            for l in range(2):
                out[t, l] = (
                    increment[:, l * COLS : (l + 1) * COLS] + mean[t, l : l + 1, :]
                ).astype(BF16)
            tiles.append(t)
        settle(pad)
        for t in tiles:
            send_tile(t)

    def advance(k, carry):
        @pl.when(k < 4)
        def _():
            solve(lax.rem(lax.div(gy, 2) + k, 4))

        @pl.when(k == 0)
        def _():
            pl.semaphore_wait(barrier, PEERS - 1)

        @pl.when(k > 0)
        def _():
            update(lax.rem(lax.div(gy, 2) + k + 3, 4))

        return carry

    lax.fori_loop(0, 5, advance, 0)
    o_ref[me] = out[gy, :, pl.ds(pl.multiple_of(mem * LOCAL, LOCAL), LOCAL), :]
    for_each_peer(mem, gy, lambda k, om, og: piece(og, om, k).wait_recv())
    for_each_peer(mem, gy, lambda k, om, og: piece(og, om, k).wait_send())


def analysis(strip, cells, values, errors):
    vm = pltpu.VMEM
    return pl.pallas_call(
        analysis_kernel,
        out_shape=jax.ShapeDtypeStruct((ROWS, 2, LOCAL, COLS), BF16),
        in_specs=[pl.BlockSpec(memory_space=pltpu.VMEM)] * 4,
        out_specs=pl.BlockSpec(memory_space=pltpu.VMEM),
        scratch_shapes=[
            vm((8, MEMS, MEMS), BF16), vm((8, 8, COLS), F32), vm((4, MEMS, COLS), F32),
            vm((4, 1, COLS), F32), vm((4, MEMS, MEMS), BF16), vm((8, 2, MEMS, COLS), BF16), vm((8, COLS), F32),
            pltpu.SemaphoreType.DMA((PEERS,)), pltpu.SemaphoreType.DMA((PEERS,)),
        ],
        compiler_params=pltpu.CompilerParams(collective_id=1, has_side_effects=True),
        name="analysis",
    )(strip, cells, values, errors)


def on_device(prior_sample_set, flow_speeds, observed_cells, observed_values, error_variance):
    strip = forecast(prior_sample_set, flow_speeds.reshape(4, ROWS, COLS))
    shape = (4, 1, COLS)
    result = analysis(
        strip,
        observed_cells.reshape(shape),
        observed_values.reshape(shape),
        error_variance.reshape(shape),
    )
    return jnp.transpose(result, (2, 1, 0, 3))


def solution(mesh):
    in_specs = (
        P("mem", None, "gx", "gy"),
        P(None, None, "gx", "gy"),
        P("gx", "gy", "mem", None, None),
        P("gx", "gy", "mem", None, None),
        P("gx", "gy", "mem", None, None),
    )
    out_specs = P("mem", None, "gx", "gy")
    return jax.shard_map(
        on_device, mesh=mesh, in_specs=in_specs, out_specs=out_specs, check_vma=False
    )
```
